512 devices in a mesh: fsdp: 64 (over z, y_hi, core), tensor: 8 (over y_lo, x).
Axes of the slice: x: 4, y: 8 (y_hi: 4, y_lo: 2; y = y_hi * 2 + y_lo), z: 8, core: 2. Of those that a mesh axis runs over, the one named last changes fastest.
Arguments:
- hidden: bfloat16 [256, 8192], P(None, 'fsdp'), may hold values from -128 to 128
- head_weight: bfloat16 [65536, 8192], P('tensor', 'fsdp'), may hold values from -1 to 1
- targets: int32 [256], replicated, may hold values from 0 to 65535
Outputs:
- logprob: float32 [256], replicated
- greedy_gap: float32 [256], replicated
The draws below stay inside these ranges and needn't reach their ends.
All inputs are finite; a program needn't handle non-finite values.
Results may differ from the reference program's by a relative error of at most 0.0003.
Values may be sent and summed in bfloat16 or wider, within the bound.
No kernel may reach another device: no remote copies, remote signals or barrier semaphores. Data moves between devices by JAX's collectives and lax.ppermute only.
A program may use at most 64 MiB of HBM per device.

```python
import jax
import jax.numpy as jnp
from jax import lax

D = 8192
VOCAB = 65536
TOKENS = 256
N_TENSOR = 8


def head_row(base_key, vocab_index):
    row_values = jax.random.normal(jax.random.fold_in(jax.random.fold_in(base_key, 7), vocab_index), (D,), jnp.float32)
    return row_values / jnp.sqrt(jnp.sum(row_values * row_values))


def draw_head_weight(key, part):

    def one_row(vocab_index):
        return head_row(key, vocab_index)
    return jax.vmap(one_row)(jnp.arange(VOCAB, dtype=jnp.int32)).astype(jnp.bfloat16)


def draw_hidden(key, part):
    own_key = jax.random.fold_in(key, 11)
    subkeys = jax.random.split(own_key, 2)
    values = jax.random.normal(subkeys[1], (TOKENS, D), jnp.float32) * 3.0
    return jnp.clip(values, -128.0, 128.0).astype(jnp.bfloat16)


def set_ends(result, rng, low, largest):
    longest = result.shape.index(max(result.shape))
    spots = []
    for shift in (0, 1):
        where = [jax.random.randint(jax.random.fold_in(rng, axis), (), 0, length) for axis, length in enumerate(result.shape)]
        where[longest] = (where[longest] + shift) % result.shape[longest]
        spots.append(tuple(where))
    return result.at[spots[0]].set(low).at[spots[1]].set(largest)


def setup_inputs(seed: int = 0) -> dict:
    key_of = jax.random.split(jax.random.key(seed), 4)
    hidden = draw_hidden(jax.random.fold_in(key_of[3], 71), 0)
    head_weight = draw_head_weight(jax.random.fold_in(key_of[3], 71), 0)
    targets = set_ends(jax.random.randint(key_of[2], (TOKENS,), 0, VOCAB), jax.random.fold_in(key_of[2], 1), 0, VOCAB - 1).astype(jnp.int32)
    return dict(hidden=hidden, head_weight=head_weight, targets=targets)


def reference(hidden, head_weight, targets):
    block_rows = VOCAB // N_TENSOR
    stacked = head_weight.reshape(N_TENSOR, block_rows, D)

    def visit(state, inputs):
        peak_logit, expsum, target_logit = state
        head_block, block_index = inputs
        logits = jnp.dot(hidden, head_block.T, preferred_element_type=jnp.float32)
        vocab_ids = block_index * block_rows + jnp.arange(block_rows, dtype=jnp.int32)
        new_peak = jnp.maximum(peak_logit, jnp.max(logits, axis=1))
        expsum = expsum * jnp.exp(peak_logit - new_peak) + jnp.sum(jnp.exp(logits - new_peak[:, None]), axis=1)
        matches = vocab_ids[None, :] == targets[:, None]
        target_logit = target_logit + jnp.sum(jnp.where(matches, logits, jnp.zeros_like(logits)), axis=1)
        return (new_peak, expsum, target_logit), None

    start_state = (jnp.full((TOKENS,), -jnp.inf, jnp.float32), jnp.zeros((TOKENS,), jnp.float32), jnp.zeros((TOKENS,), jnp.float32))
    final_state, _ = lax.scan(visit, start_state, (stacked, jnp.arange(N_TENSOR, dtype=jnp.int32)))
    peak_logit, expsum, target_logit = final_state
    logprob = target_logit - peak_logit - jnp.log(expsum)
    greedy_gap = target_logit - peak_logit
    return logprob, greedy_gap
```

```python
import jax
import jax.numpy as jnp
from jax import lax
from jax.experimental import pallas as pl
from jax.experimental.pallas import tpu as pltpu
from jax.sharding import Mesh
from jax.sharding import PartitionSpec as P

Z, Y, CORE, YL, X = "fsdp_0", "fsdp_1", "fsdp_2", "tensor_0", "tensor_1"
FSDP = (Z, Y, CORE)
TENSOR = (YL, X)
OWNERS = (Z, Y)
FIRST = (Z, CORE)
SECOND = (Y, YL, X)
LANES = 128


def encode(value):
    square = value * jnp.abs(value)
    return (square * jnp.abs(square)).astype(jnp.bfloat16)


def decode(code):
    code = code.astype(jnp.float32)
    root = lax.rsqrt(lax.rsqrt(jnp.abs(code)))
    return jnp.where(code < 0, -root, root)


def partial_kernel(_, own_ref, their_ref, own_hidden_ref, their_hidden_ref, out_ref):
    rows = jnp.concatenate([own_ref[...], their_ref[...]], axis=1)
    hidden = jnp.concatenate([own_hidden_ref[...], their_hidden_ref[...]], axis=1)
    logits = lax.dot_general(
        rows, hidden, (((1,), (1,)), ((), ())), preferred_element_type=jnp.float32
    )
    out_ref[...] = encode(logits)


def partial_logits(core, head_weight, hidden, swapped):
    half = head_weight.shape[0] // 2
    tokens, depth = hidden.shape
    block = min(512, half)
    steps = half // block
    return pl.pallas_call(
        partial_kernel,
        grid_spec=pltpu.PrefetchScalarGridSpec(
            num_scalar_prefetch=1,
            grid=(steps,),
            in_specs=[
                pl.BlockSpec((block, depth), lambda i, c: (c[0] * steps + i, 0)),
                pl.BlockSpec((block, depth), lambda i, c: (i, 0)),
                pl.BlockSpec((tokens, depth), lambda i, c: (0, 0)),
                pl.BlockSpec((tokens, depth), lambda i, c: (half // tokens, 0)),
            ],
            out_specs=pl.BlockSpec((block, tokens), lambda i, c: (i, 0)),
        ),
        out_shape=jax.ShapeDtypeStruct((half, tokens), jnp.bfloat16),
        name="partial_logits",
    )(core, head_weight, swapped, hidden, swapped)


def put_stats(out_ref, peak, expsum, target):
    zeros = jnp.zeros((2, LANES), jnp.float32)
    packed = jnp.concatenate([peak, expsum, target, zeros], axis=0)
    for k in range(out_ref.shape[0]):
        out_ref[k] = packed


def two_rows(row):
    return jnp.concatenate([row[:, :LANES], row[:, LANES:]], axis=0)


def stats_kernel(codes_ref, target_ref, out_ref, logits_ref):
    peers, rows, tokens = codes_ref.shape
    step = 32

    def add_rows(k, peak):
        at = pl.ds(pl.multiple_of(k * step, step), step)
        total = decode(codes_ref[0, at, :])
        for peer in range(1, peers):
            total = total + decode(codes_ref[peer, at, :])
        logits_ref[at, :] = total
        return jnp.maximum(peak, jnp.max(total, axis=0, keepdims=True))

    peak = lax.fori_loop(
        0, rows // step, add_rows, jnp.full((1, tokens), -jnp.inf, jnp.float32)
    )
    expsum = jnp.sum(jnp.exp(logits_ref[...] - peak), axis=0, keepdims=True)
    put_stats(out_ref, two_rows(peak), two_rows(expsum), target_ref[...])


def combine(parts):
    peaks, expsums, targets = parts[:, 0:2], parts[:, 2:4], parts[:, 4:6]
    peak = jnp.max(peaks, axis=0)
    expsum = jnp.sum(expsums * jnp.exp(peaks - peak), axis=0)
    return peak, expsum, jnp.sum(targets, axis=0)


def combine_kernel(parts_ref, out_ref):
    put_stats(out_ref, *combine(parts_ref[...]))


def finish_kernel(parts_ref, logprob_ref, gap_ref):
    peak, expsum, target = combine(parts_ref[...])
    logprob_ref[...] = target - peak - jnp.log(expsum)
    gap_ref[...] = target - peak


def own_target(hidden, head_weight, targets):
    held = head_weight.shape[0]
    local = targets - lax.axis_index(TENSOR) * held
    rows = jnp.take(head_weight, jnp.clip(local, 0, held - 1), axis=0)
    share = jnp.sum(rows.astype(jnp.float32) * hidden.astype(jnp.float32), axis=1)
    return jnp.where((local >= 0) & (local < held), share, 0.0)


def per_device(hidden, head_weight, targets):
    held = head_weight.shape[0]
    tokens = hidden.shape[0]
    half = held // 2
    core = lax.axis_index(CORE)
    others = lax.dynamic_slice_in_dim(head_weight, (1 - core) * half, half, axis=0)
    swapped = lax.ppermute(jnp.concatenate([others, hidden]), CORE, [(0, 1), (1, 0)])
    codes = partial_logits(core.reshape(1).astype(jnp.int32), head_weight, hidden, swapped)
    peers = lax.axis_size(OWNERS)
    codes = lax.all_to_all(codes.reshape(peers, half // peers, tokens), OWNERS, 0, 0)
    target = own_target(hidden, head_weight, targets).reshape(2, LANES)
    stats = pl.pallas_call(
        stats_kernel,
        out_shape=jax.ShapeDtypeStruct((lax.axis_size(FIRST), 8, LANES), jnp.float32),
        scratch_shapes=[pltpu.VMEM((half // peers, tokens), jnp.float32)],
        name="stats",
    )(codes, target)
    stats = lax.all_to_all(stats, FIRST, 0, 0)
    stats = pl.pallas_call(
        combine_kernel,
        out_shape=jax.ShapeDtypeStruct((lax.axis_size(SECOND), 8, LANES), jnp.float32),
        name="combine",
    )(stats)
    stats = lax.all_to_all(stats, SECOND, 0, 0)
    pair = jax.ShapeDtypeStruct((2, LANES), jnp.float32)
    logprob, gap = pl.pallas_call(finish_kernel, out_shape=(pair, pair), name="finish")(stats)
    return logprob.reshape(tokens), gap.reshape(tokens)


def solution(mesh):
    torus = Mesh(mesh.devices.reshape(8, 4, 2, 2, 4), FSDP + TENSOR)
    placed = (P(None, FSDP), P(TENSOR, FSDP), P())
    return jax.shard_map(
        per_device, mesh=torus, in_specs=placed, out_specs=(P(), P()), check_vma=False
    )
```

```python
import jax
import jax.numpy as jnp
from jax import lax
from jax.experimental import pallas as pl
from jax.experimental.pallas import tpu as pltpu
from jax.sharding import Mesh
from jax.sharding import PartitionSpec as P

Z, Y, CORE, YL, X = "fsdp_0", "fsdp_1", "fsdp_2", "tensor_0", "tensor_1"
FSDP = (Z, Y, CORE)
TENSOR = (YL, X)
OWNERS = (Z, Y)
FIRST = (Z, CORE)
SECOND = (Y, YL, X)
LANES = 128


def encode(value):
    square = value * jnp.abs(value)
    return (square * jnp.abs(square)).astype(jnp.bfloat16)


def decode(code):
    code = code.astype(jnp.float32)
    root = lax.rsqrt(lax.rsqrt(jnp.abs(code)))
    return jnp.where(code < 0, -root, root)


def partial_kernel(own_ref, swapped_ref, hidden_ref, out_ref):
    half, depth = own_ref.shape
    tokens = hidden_ref.shape[0]
    hidden = jnp.concatenate([hidden_ref[...], swapped_ref[half : half + tokens, :]], axis=1)
    step = min(512, half)

    def add_rows(k, carry):
        at = pl.ds(pl.multiple_of(k * step, step), step)
        rows = jnp.concatenate([own_ref[at, :], swapped_ref[at, :]], axis=1)
        logits = lax.dot_general(
            rows, hidden, (((1,), (1,)), ((), ())), preferred_element_type=jnp.float32
        )
        out_ref[at, :] = encode(logits)
        return carry

    lax.fori_loop(0, half // step, add_rows, 0)


def local_call(kernel, name, out, *operands, place=pltpu.VMEM, **more):
    results = [place(shape, dtype) for shape, dtype in out]
    specs = [pl.BlockSpec(memory_space=pltpu.VMEM)] * len(operands)
    operands = [pltpu.with_memory_space_constraint(x, pltpu.VMEM) for x in operands]
    params = pltpu.CompilerParams(vmem_limit_bytes=16 * 2**20)
    return pl.pallas_call(
        kernel, in_specs=specs, out_shape=results, name=name, compiler_params=params, **more
    )(*operands)


def put_stats(out_ref, peak, expsum, target):
    zeros = jnp.zeros((2, LANES), jnp.float32)
    packed = jnp.concatenate([peak, expsum, target, zeros], axis=0)
    for k in range(out_ref.shape[0]):
        out_ref[k] = packed


def two_rows(row):
    return jnp.concatenate([row[:, :LANES], row[:, LANES:]], axis=0)


def stats_kernel(codes_ref, target_ref, out_ref, logits_ref):
    peers, rows, tokens = codes_ref.shape
    step = 32

    def add_rows(k, peak):
        at = pl.ds(pl.multiple_of(k * step, step), step)
        total = decode(codes_ref[0, at, :])
        for peer in range(1, peers):
            total = total + decode(codes_ref[peer, at, :])
        logits_ref[at, :] = total
        return jnp.maximum(peak, jnp.max(total, axis=0, keepdims=True))

    peak = lax.fori_loop(
        0, rows // step, add_rows, jnp.full((1, tokens), -jnp.inf, jnp.float32)
    )
    expsum = jnp.sum(jnp.exp(logits_ref[...] - peak), axis=0, keepdims=True)
    put_stats(out_ref, two_rows(peak), two_rows(expsum), target_ref[...])


def combine(parts):
    peaks, expsums, targets = parts[:, 0:2], parts[:, 2:4], parts[:, 4:6]
    peak = jnp.max(peaks, axis=0)
    expsum = jnp.sum(expsums * jnp.exp(peaks - peak), axis=0)
    return peak, expsum, jnp.sum(targets, axis=0)


def combine_kernel(parts_ref, out_ref):
    put_stats(out_ref, *combine(parts_ref[...]))


def finish_kernel(parts_ref, logprob_ref, gap_ref):
    peak, expsum, target = combine(parts_ref[...])
    logprob_ref[...] = target - peak - jnp.log(expsum)
    gap_ref[...] = target - peak


def own_target(hidden, head_weight, targets):
    held = head_weight.shape[0]
    local = targets - lax.axis_index(TENSOR) * held
    rows = jnp.take(head_weight, jnp.clip(local, 0, held - 1), axis=0)
    share = jnp.sum(rows.astype(jnp.float32) * hidden.astype(jnp.float32), axis=1)
    return jnp.where((local >= 0) & (local < held), share, 0.0)


def per_device(hidden, head_weight, targets):
    held = head_weight.shape[0]
    tokens = hidden.shape[0]
    half = held // 2
    peers = lax.axis_size(OWNERS)
    core = lax.axis_index(CORE)
    others = lax.dynamic_slice_in_dim(head_weight, (1 - core) * half, half, axis=0)
    own = lax.dynamic_slice_in_dim(head_weight, core * half, half, axis=0)
    swapped = lax.ppermute(jnp.concatenate([others, hidden]), CORE, [(0, 1), (1, 0)])
    (codes,) = local_call(
        partial_kernel, "partial", [((half, tokens), jnp.bfloat16)], own, swapped, hidden
    )
    target = own_target(hidden, head_weight, targets).reshape(2, LANES)
    codes, target = lax.optimization_barrier((codes, target))
    codes = lax.all_to_all(codes.reshape(peers, half // peers, tokens), OWNERS, 0, 0)
    (stats,) = local_call(
        stats_kernel,
        "stats",
        [((lax.axis_size(FIRST), 8, LANES), jnp.float32)],
        codes,
        target,
        scratch_shapes=[pltpu.VMEM((half // peers, tokens), jnp.float32)],
    )
    stats = lax.all_to_all(stats, FIRST, 0, 0)
    (stats,) = local_call(
        combine_kernel, "combine", [((lax.axis_size(SECOND), 8, LANES), jnp.float32)], stats
    )
    stats = lax.all_to_all(stats, SECOND, 0, 0)
    logprob, gap = local_call(
        finish_kernel,
        "finish",
        [((2, LANES), jnp.float32)] * 2,
        stats,
        place=jax.ShapeDtypeStruct,
    )
    return logprob.reshape(tokens), gap.reshape(tokens)


def solution(mesh):
    torus = Mesh(mesh.devices.reshape(8, 4, 2, 2, 4), FSDP + TENSOR)
    placed = (P(None, FSDP), P(TENSOR, FSDP), P())
    return jax.shard_map(
        per_device, mesh=torus, in_specs=placed, out_specs=(P(), P()), check_vma=False
    )
```

```python
import jax
import jax.numpy as jnp
from jax import lax
from jax.experimental import pallas as pl
from jax.experimental.pallas import tpu as pltpu
from jax.sharding import Mesh
from jax.sharding import PartitionSpec as P

Z, Y, CORE, YL, X = "fsdp_0", "fsdp_1", "fsdp_2", "tensor_0", "tensor_1"
FSDP = (Z, Y, CORE)
TENSOR = (YL, X)
OWNERS = (Y, Z)
FIRST = (Z, CORE)
SECOND = (Y, YL, X)
LANES = 128


def encode(value):
    square = value * jnp.abs(value)
    return (square * jnp.abs(square)).astype(jnp.bfloat16)


def decode(code):
    code = code.astype(jnp.float32)
    root = lax.rsqrt(lax.rsqrt(jnp.abs(code)))
    return jnp.where(code < 0, -root, root)


def partial_kernel(own_ref, swapped_ref, hidden_ref, out_ref):
    half, depth = own_ref.shape
    tokens = hidden_ref.shape[0]
    hidden = jnp.concatenate([hidden_ref[...], swapped_ref[half : half + tokens, :]], axis=1)
    step = min(512, half)

    def add_rows(k, carry):
        at = pl.ds(pl.multiple_of(k * step, step), step)
        rows = jnp.concatenate([own_ref[at, :], swapped_ref[at, :]], axis=1)
        logits = lax.dot_general(
            rows, hidden, (((1,), (1,)), ((), ())), preferred_element_type=jnp.float32
        )
        out_ref[at, :] = encode(logits)
        return carry

    lax.fori_loop(0, half // step, add_rows, 0)


def local_call(kernel, name, out, *operands, place=pltpu.VMEM, **more):
    results = [place(shape, dtype) for shape, dtype in out]
    specs = [pl.BlockSpec(memory_space=pltpu.VMEM)] * len(operands)
    operands = [pltpu.with_memory_space_constraint(x, pltpu.VMEM) for x in operands]
    params = pltpu.CompilerParams(vmem_limit_bytes=16 * 2**20)
    return pl.pallas_call(
        kernel, in_specs=specs, out_shape=results, name=name, compiler_params=params, **more
    )(*operands)


def put_stats(out_ref, peak, expsum, target):
    zeros = jnp.zeros((2, LANES), jnp.float32)
    packed = jnp.concatenate([peak, expsum, target, zeros], axis=0)
    for k in range(out_ref.shape[0]):
        out_ref[k] = packed


def two_rows(row):
    return jnp.concatenate([row[:, :LANES], row[:, LANES:]], axis=0)


def stats_kernel(codes_ref, target_ref, out_ref, logits_ref):
    peers, rows, tokens = codes_ref.shape
    step = 32

    def add_rows(k, peak):
        at = pl.ds(pl.multiple_of(k * step, step), step)
        total = decode(codes_ref[0, at, :])
        for peer in range(1, peers):
            total = total + decode(codes_ref[peer, at, :])
        logits_ref[at, :] = total
        return jnp.maximum(peak, jnp.max(total, axis=0, keepdims=True))

    peak = lax.fori_loop(
        0, rows // step, add_rows, jnp.full((1, tokens), -jnp.inf, jnp.float32)
    )
    expsum = jnp.sum(jnp.exp(logits_ref[...] - peak), axis=0, keepdims=True)
    put_stats(out_ref, two_rows(peak), two_rows(expsum), target_ref[...])


def combine(parts):
    peaks, expsums, targets = parts[:, 0:2], parts[:, 2:4], parts[:, 4:6]
    peak = jnp.max(peaks, axis=0)
    expsum = jnp.sum(expsums * jnp.exp(peaks - peak), axis=0)
    return peak, expsum, jnp.sum(targets, axis=0)


def combine_kernel(parts_ref, out_ref):
    put_stats(out_ref, *combine(parts_ref[...]))


def finish_kernel(parts_ref, logprob_ref, gap_ref):
    peak, expsum, target = combine(parts_ref[...])
    logprob_ref[...] = target - peak - jnp.log(expsum)
    gap_ref[...] = target - peak


def own_target(hidden, head_weight, targets):
    held = head_weight.shape[0]
    local = targets - lax.axis_index(TENSOR) * held
    rows = jnp.take(head_weight, jnp.clip(local, 0, held - 1), axis=0)
    share = jnp.sum(rows.astype(jnp.float32) * hidden.astype(jnp.float32), axis=1)
    return jnp.where((local >= 0) & (local < held), share, 0.0)


def per_device(hidden, head_weight, targets):
    held = head_weight.shape[0]
    tokens = hidden.shape[0]
    half = held // 2
    peers = lax.axis_size(OWNERS)
    core = lax.axis_index(CORE)
    others = lax.dynamic_slice_in_dim(head_weight, (1 - core) * half, half, axis=0)
    own = lax.dynamic_slice_in_dim(head_weight, core * half, half, axis=0)
    swapped = lax.ppermute(jnp.concatenate([others, hidden]), CORE, [(0, 1), (1, 0)])
    (codes,) = local_call(
        partial_kernel, "partial", [((half, tokens), jnp.bfloat16)], own, swapped, hidden
    )
    target = own_target(hidden, head_weight, targets).reshape(2, LANES)
    codes, target = lax.optimization_barrier((codes, target))
    codes = lax.all_to_all(codes.reshape(peers, half // peers, tokens), OWNERS, 0, 0)
    (stats,) = local_call(
        stats_kernel,
        "stats",
        [((lax.axis_size(FIRST), 8, LANES), jnp.float32)],
        codes,
        target,
        scratch_shapes=[pltpu.VMEM((half // peers, tokens), jnp.float32)],
    )
    stats = lax.all_to_all(stats, FIRST, 0, 0)
    (stats,) = local_call(
        combine_kernel, "combine", [((lax.axis_size(SECOND), 8, LANES), jnp.float32)], stats
    )
    stats = lax.all_to_all(stats, SECOND, 0, 0)
    logprob, gap = local_call(
        finish_kernel,
        "finish",
        [((2, LANES), jnp.float32)] * 2,
        stats,
        place=jax.ShapeDtypeStruct,
    )
    return logprob.reshape(tokens), gap.reshape(tokens)


def solution(mesh):
    torus = Mesh(mesh.devices.reshape(8, 4, 2, 2, 4), FSDP + TENSOR)
    placed = (P(None, FSDP), P(TENSOR, FSDP), P())
    return jax.shard_map(
        per_device, mesh=torus, in_specs=placed, out_specs=(P(), P()), check_vma=False
    )
```

```python
import functools

import jax
import jax.numpy as jnp
from jax import lax
from jax.experimental import pallas as pl
from jax.experimental.pallas import tpu as pltpu
from jax.sharding import Mesh
from jax.sharding import PartitionSpec as P

Z, Y, CORE, YL, X = "fsdp_0", "fsdp_1", "fsdp_2", "tensor_0", "tensor_1"
FSDP = (Z, Y, CORE)
TENSOR = (YL, X)
ALL = FSDP + TENSOR
FIRST = (Z, CORE)
SECOND = (Y, YL, X)
LANES = 128


REACH = 25


def encode(value):
    square = value * value
    return (square * square * value).astype(jnp.bfloat16)


def decode(code):
    code = code.astype(jnp.float32)
    size = jnp.abs(code)
    root = jnp.exp2(jnp.log2(jnp.maximum(size, 2.0**-126)) * 0.2)
    return jnp.where(code < 0, -root, jnp.where(code > 0, root, 0.0))


def decoded_sum(codes_ref, at):
    total = decode(codes_ref[0, at, :])
    for peer in range(1, codes_ref.shape[0]):
        total = total + decode(codes_ref[peer, at, :])
    return total


def partial_kernel(scale, own_ref, swapped_ref, hidden_ref, out_ref):
    half, depth = own_ref.shape
    tokens = hidden_ref.shape[0]
    hidden = jnp.concatenate([hidden_ref[...], swapped_ref[half : half + tokens, :]], axis=1)
    step = min(512, half)

    def add_rows(k, carry):
        at = pl.ds(pl.multiple_of(k * step, step), step)
        rows = jnp.concatenate([own_ref[at, :], swapped_ref[at, :]], axis=1)
        logits = lax.dot_general(
            rows, hidden, (((1,), (1,)), ((), ())), preferred_element_type=jnp.float32
        )
        out_ref[at, :] = encode(logits * scale)
        return carry

    lax.fori_loop(0, half // step, add_rows, 0)


def local_call(kernel, name, out, *operands, place=pltpu.VMEM, **more):
    results = [place(shape, dtype) for shape, dtype in out]
    specs = [pl.BlockSpec(memory_space=pltpu.VMEM)] * len(operands)
    operands = [pltpu.with_memory_space_constraint(x, pltpu.VMEM) for x in operands]
    params = pltpu.CompilerParams(vmem_limit_bytes=16 * 2**20)
    return pl.pallas_call(
        kernel, in_specs=specs, out_shape=results, name=name, compiler_params=params, **more
    )(*operands)


def put_stats(out_ref, peak, expsum, target):
    zeros = jnp.zeros((2, LANES), jnp.float32)
    packed = jnp.concatenate([peak, expsum, target, zeros], axis=0)
    for k in range(out_ref.shape[0]):
        out_ref[k] = packed


def two_rows(row):
    return jnp.concatenate([row[:, :LANES], row[:, LANES:]], axis=0)


def sum_kernel(scale, codes_ref, out_ref):
    step = 32

    def add_rows(k, carry):
        at = pl.ds(pl.multiple_of(k * step, step), step)
        out_ref[at, :] = encode(decoded_sum(codes_ref, at) * scale)
        return carry

    lax.fori_loop(0, out_ref.shape[0] // step, add_rows, 0)


def stats_kernel(scale, codes_ref, target_ref, out_ref, logits_ref):
    rows, tokens = logits_ref.shape
    step = 32

    def add_rows(k, peak):
        at = pl.ds(pl.multiple_of(k * step, step), step)
        total = decoded_sum(codes_ref, at) * scale
        logits_ref[at, :] = total
        return jnp.maximum(peak, jnp.max(total, axis=0, keepdims=True))

    peak = lax.fori_loop(
        0, rows // step, add_rows, jnp.full((1, tokens), -jnp.inf, jnp.float32)
    )
    expsum = jnp.sum(jnp.exp(logits_ref[...] - peak), axis=0, keepdims=True)
    put_stats(out_ref, two_rows(peak), two_rows(expsum), target_ref[...])


def combine(parts):
    peaks, expsums, targets = parts[:, 0:2], parts[:, 2:4], parts[:, 4:6]
    peak = jnp.max(peaks, axis=0)
    expsum = jnp.sum(expsums * jnp.exp(peaks - peak), axis=0)
    return peak, expsum, jnp.sum(targets, axis=0)


def combine_kernel(parts_ref, out_ref):
    put_stats(out_ref, *combine(parts_ref[...]))


def finish_kernel(parts_ref, logprob_ref, gap_ref):
    peak, expsum, target = combine(parts_ref[...])
    logprob_ref[...] = target - peak - jnp.log(expsum)
    gap_ref[...] = target - peak


def own_target(hidden, head_weight, targets):
    held = head_weight.shape[0]
    local = targets - lax.axis_index(TENSOR) * held
    rows = jnp.take(head_weight, jnp.clip(local, 0, held - 1), axis=0)
    share = jnp.sum(rows.astype(jnp.float32) * hidden.astype(jnp.float32), axis=1)
    return jnp.where((local >= 0) & (local < held), share, 0.0)


def round_groups(deep, high, tensor):
    def at(z, y, core, rest):
        return ((z * high + y) * 2 + core) * tensor + rest

    one, two = [], []
    for rest in range(tensor):
        for parity in range(2):
            for y in range(high):
                one.append([at(z, y, 0, rest) for z in range(parity, deep, 2)])
        for z in range(deep):
            one.append([at(z, y, 1, rest) for y in range(high)])
        for pair in range(0, deep, 2):
            two.append([at(z, y, 0, rest) for y in range(high) for z in (pair, pair + 1)])
        for y in range(high):
            two.append([at(z, y, 1, rest) for z in range(deep)])
    return one, two


def per_device(hidden, head_weight, targets):
    held = head_weight.shape[0]
    tokens = hidden.shape[0]
    half = held // 2
    deep, high = lax.axis_size(Z), lax.axis_size(Y)
    one, two = round_groups(deep, high, lax.axis_size(TENSOR))
    core = lax.axis_index(CORE)
    others = lax.dynamic_slice_in_dim(head_weight, (1 - core) * half, half, axis=0)
    own = lax.dynamic_slice_in_dim(head_weight, core * half, half, axis=0)
    swapped = lax.ppermute(jnp.concatenate([others, hidden]), CORE, [(0, 1), (1, 0)])
    (codes,) = local_call(
        functools.partial(partial_kernel, 2.0 ** (REACH - 15)),
        "partial",
        [((half, tokens), jnp.bfloat16)],
        own,
        swapped,
        hidden,
    )
    target = own_target(hidden, head_weight, targets).reshape(2, LANES)
    codes, target = lax.optimization_barrier((codes, target))
    rows = half // high
    codes = codes.reshape(high, rows, tokens)
    codes = lax.all_to_all(codes, ALL, 0, 0, axis_index_groups=one)
    (codes,) = local_call(
        functools.partial(sum_kernel, 2.0**-2), "sum", [((rows, tokens), jnp.bfloat16)], codes
    )
    codes = codes.reshape(deep, rows // deep, tokens)
    codes = lax.all_to_all(codes, ALL, 0, 0, axis_index_groups=two)
    (stats,) = local_call(
        functools.partial(stats_kernel, 2.0 ** (17 - REACH)),
        "stats",
        [((lax.axis_size(FIRST), 8, LANES), jnp.float32)],
        codes,
        target,
        scratch_shapes=[pltpu.VMEM((rows // deep, tokens), jnp.float32)],
    )
    stats = lax.all_to_all(stats, FIRST, 0, 0)
    (stats,) = local_call(
        combine_kernel, "combine", [((lax.axis_size(SECOND), 8, LANES), jnp.float32)], stats
    )
    stats = lax.all_to_all(stats, SECOND, 0, 0)
    logprob, gap = local_call(
        finish_kernel,
        "finish",
        [((2, LANES), jnp.float32)] * 2,
        stats,
        place=jax.ShapeDtypeStruct,
    )
    return logprob.reshape(tokens), gap.reshape(tokens)


def solution(mesh):
    torus = Mesh(mesh.devices.reshape(8, 4, 2, 2, 4), FSDP + TENSOR)
    placed = (P(None, FSDP), P(TENSOR, FSDP), P())
    return jax.shard_map(
        per_device, mesh=torus, in_specs=placed, out_specs=(P(), P()), check_vma=False
    )
```

```python
import functools

import jax
import jax.numpy as jnp
from jax import lax
from jax.experimental import pallas as pl
from jax.experimental.pallas import tpu as pltpu
from jax.sharding import Mesh
from jax.sharding import PartitionSpec as P

Z, Y, CORE, YL, X = "fsdp_0", "fsdp_1", "fsdp_2", "tensor_0", "tensor_1"
FSDP = (Z, Y, CORE)
TENSOR = (YL, X)
ALL = FSDP + TENSOR
FIRST = (CORE, Z)
SECOND = (X, YL, Y)
LANES = 128


REACH = 20


def encode(value):
    cube = value * value * value
    return (cube * jnp.abs(cube)).astype(jnp.bfloat16)


def decode(code):
    code = code.astype(jnp.float32)
    size = jnp.abs(code)
    root = jnp.exp2(jnp.log2(jnp.maximum(size, 2.0**-126)) * (1 / 6))
    return jnp.where(code < 0, -root, jnp.where(code > 0, root, 0.0))


def decoded_sum(codes_ref, at):
    total = decode(codes_ref[0, at, :])
    for peer in range(1, codes_ref.shape[0]):
        total = total + decode(codes_ref[peer, at, :])
    return total


def partial_kernel(scale, own_ref, swapped_ref, hidden_ref, out_ref):
    half, depth = own_ref.shape
    tokens = hidden_ref.shape[0]
    hidden = jnp.concatenate([hidden_ref[...], swapped_ref[half : half + tokens, :]], axis=1)
    step = min(512, half)

    def add_rows(k, carry):
        at = pl.ds(pl.multiple_of(k * step, step), step)
        rows = jnp.concatenate([own_ref[at, :], swapped_ref[at, :]], axis=1)
        logits = lax.dot_general(
            rows, hidden, (((1,), (1,)), ((), ())), preferred_element_type=jnp.float32
        )
        out_ref[at, :] = encode(logits * scale)
        return carry

    lax.fori_loop(0, half // step, add_rows, 0, unroll=True)


def local_call(kernel, name, out, *operands, place=pltpu.VMEM, **more):
    results = [place(shape, dtype) for shape, dtype in out]
    specs = [pl.BlockSpec(memory_space=pltpu.VMEM)] * len(operands)
    operands = [pltpu.with_memory_space_constraint(x, pltpu.VMEM) for x in operands]
    params = pltpu.CompilerParams(vmem_limit_bytes=16 * 2**20)
    return pl.pallas_call(
        kernel, in_specs=specs, out_shape=results, name=name, compiler_params=params, **more
    )(*operands)


def put_stats(out_ref, peak, expsum, target):
    zeros = jnp.zeros((2, LANES), jnp.float32)
    packed = jnp.concatenate([peak, expsum, target, zeros], axis=0)
    for k in range(out_ref.shape[0]):
        out_ref[k] = packed


def two_rows(row):
    return jnp.concatenate([row[:, :LANES], row[:, LANES:]], axis=0)


def sum_kernel(scale, codes_ref, out_ref):
    step = 32

    def add_rows(k, carry):
        at = pl.ds(pl.multiple_of(k * step, step), step)
        out_ref[at, :] = encode(decoded_sum(codes_ref, at) * scale)
        return carry

    lax.fori_loop(0, out_ref.shape[0] // step, add_rows, 0, unroll=4)


def stats_kernel(scale, codes_ref, target_row_ref, out_ref, logits_ref):
    rows, tokens = logits_ref.shape
    step = 32

    def add_rows(k, state):
        peak, target = state
        at = pl.ds(pl.multiple_of(k * step, step), step)
        total = decoded_sum(codes_ref, at) * scale
        logits_ref[at, :] = total
        peak = jnp.maximum(peak, jnp.max(total, axis=0, keepdims=True))
        row = lax.broadcasted_iota(jnp.int32, total.shape, 0) + k * step
        matched = jnp.where(row == target_row_ref[...], total, 0.0)
        return peak, target + jnp.sum(matched, axis=0, keepdims=True)

    start = jnp.full((1, tokens), -jnp.inf, jnp.float32), jnp.zeros((1, tokens), jnp.float32)
    peak, target = lax.fori_loop(0, rows // step, add_rows, start, unroll=True)
    expsum = jnp.sum(jnp.exp(logits_ref[...] - peak), axis=0, keepdims=True)
    put_stats(out_ref, two_rows(peak), two_rows(expsum), two_rows(target))


def combine(parts):
    peaks, expsums, targets = parts[:, 0:2], parts[:, 2:4], parts[:, 4:6]
    peak = jnp.max(peaks, axis=0)
    expsum = jnp.sum(expsums * jnp.exp(peaks - peak), axis=0)
    return peak, expsum, jnp.sum(targets, axis=0)


def combine_kernel(parts_ref, out_ref):
    put_stats(out_ref, *combine(parts_ref[...]))


def finish_kernel(parts_ref, logprob_ref, gap_ref):
    peak, expsum, target = combine(parts_ref[...])
    logprob_ref[...] = target - peak - jnp.log(expsum)
    gap_ref[...] = target - peak


def round_groups(deep, high, tensor):
    def at(z, y, core, rest):
        return ((z * high + y) * 2 + core) * tensor + rest

    one, two = [], []
    for rest in range(tensor):
        for parity in range(2):
            for y in range(high):
                one.append([at(z, y, 0, rest) for z in range(parity, deep, 2)])
        for z in range(deep):
            one.append([at(z, y, 1, rest) for y in range(high)])
        for pair in range(0, deep, 2):
            two.append([at(z, y, 0, rest) for z in (pair, pair + 1) for y in range(high)])
        for y in range(high):
            two.append([at(z, y, 1, rest) for z in range(deep)])
    return one, two


def per_device(hidden, head_weight, targets):
    held = head_weight.shape[0]
    tokens = hidden.shape[0]
    half = held // 2
    deep, high = lax.axis_size(Z), lax.axis_size(Y)
    one, two = round_groups(deep, high, lax.axis_size(TENSOR))
    core = lax.axis_index(CORE)
    others = lax.dynamic_slice_in_dim(head_weight, (1 - core) * half, half, axis=0)
    own = lax.dynamic_slice_in_dim(head_weight, core * half, half, axis=0)
    swapped = lax.ppermute(jnp.concatenate([others, hidden]), CORE, [(0, 1), (1, 0)])
    (codes,) = local_call(
        functools.partial(partial_kernel, 2.0 ** (REACH - 15)),
        "partial",
        [((half, tokens), jnp.bfloat16)],
        own,
        swapped,
        hidden,
    )
    rows = half // high
    z, y = lax.axis_index(Z), lax.axis_index(Y)
    chunk = jnp.where(core == 0, z // 2, y)
    piece = jnp.where(core == 0, z % 2 * high + y, z)
    first_row = lax.axis_index(TENSOR) * held + core * half + chunk * rows + piece * (rows // deep)
    target_row = (targets - first_row).reshape(1, tokens)
    codes, target_row = lax.optimization_barrier((codes, target_row))
    codes = codes.reshape(high, rows, tokens)
    codes = lax.all_to_all(codes, ALL, 0, 0, axis_index_groups=one)
    (codes,) = local_call(
        functools.partial(sum_kernel, 2.0**-2), "sum", [((rows, tokens), jnp.bfloat16)], codes
    )
    codes = codes.reshape(deep, rows // deep, tokens)
    codes = lax.all_to_all(codes, ALL, 0, 0, axis_index_groups=two)
    (stats,) = local_call(
        functools.partial(stats_kernel, 2.0 ** (17 - REACH)),
        "stats",
        [((lax.axis_size(FIRST), 8, LANES), jnp.float32)],
        codes,
        target_row,
        scratch_shapes=[pltpu.VMEM((rows // deep, tokens), jnp.float32)],
    )
    stats = lax.all_to_all(stats, FIRST, 0, 0)
    (stats,) = local_call(
        combine_kernel, "combine", [((lax.axis_size(SECOND), 8, LANES), jnp.float32)], stats
    )
    stats = lax.all_to_all(stats, SECOND, 0, 0)
    logprob, gap = local_call(
        finish_kernel,
        "finish",
        [((2, LANES), jnp.float32)] * 2,
        stats,
        place=jax.ShapeDtypeStruct,
    )
    return logprob.reshape(tokens), gap.reshape(tokens)


def solution(mesh):
    torus = Mesh(mesh.devices.reshape(8, 4, 2, 2, 4), FSDP + TENSOR)
    placed = (P(None, FSDP), P(TENSOR, FSDP), P())
    return jax.shard_map(
        per_device, mesh=torus, in_specs=placed, out_specs=(P(), P()), check_vma=False
    )
```

```python
import functools

import jax
import jax.numpy as jnp
from jax import lax
from jax.experimental import pallas as pl
from jax.experimental.pallas import tpu as pltpu
from jax.sharding import Mesh
from jax.sharding import PartitionSpec as P

Z, Y, CORE, YL, X = "fsdp_0", "fsdp_1", "fsdp_2", "tensor_0", "tensor_1"
FSDP = (Z, Y, CORE)
TENSOR = (YL, X)
ALL = FSDP + TENSOR
FIRST = (CORE, Z)
SECOND = (X, YL, Y)
LANES = 128


REACH = 20


def encode(value):
    cube = value * value * value
    return (cube * jnp.abs(cube)).astype(jnp.bfloat16)


def decode(code):
    code = code.astype(jnp.float32)
    size = jnp.maximum(jnp.abs(code), 2.0**-126)
    return code * jnp.exp2(jnp.log2(size) * (-5 / 6))


def decoded_sum(codes_ref, at):
    total = decode(codes_ref[0, at, :])
    for peer in range(1, codes_ref.shape[0]):
        total = total + decode(codes_ref[peer, at, :])
    return total


def pick_kernel(weight_ref, hidden_ref, out_ref, sems):
    half = weight_ref.shape[0] // 2
    start = (1 - lax.axis_index(CORE)) * half
    rows = pltpu.make_async_copy(
        weight_ref.at[pl.ds(pl.multiple_of(start, half), half)], out_ref.at[:half], sems.at[0]
    )
    features = pltpu.make_async_copy(hidden_ref, out_ref.at[half:], sems.at[1])
    rows.start()
    features.start()
    rows.wait()
    features.wait()


def pick(head_weight, hidden):
    rows = head_weight.shape[0] // 2 + hidden.shape[0]
    return pl.pallas_call(
        pick_kernel,
        in_specs=[pl.BlockSpec(memory_space=pl.ANY)] * 2,
        out_shape=pltpu.VMEM((rows, hidden.shape[1]), hidden.dtype),
        scratch_shapes=[pltpu.SemaphoreType.DMA((2,))],
        name="pick",
    )(head_weight, hidden)


def partial_kernel(scale, own_ref, swapped_ref, hidden_ref, out_ref):
    half, depth = own_ref.shape
    tokens = hidden_ref.shape[0]
    hidden = jnp.concatenate([hidden_ref[...], swapped_ref[half : half + tokens, :]], axis=1)
    step = min(512, half)

    def add_rows(k, carry):
        at = pl.ds(pl.multiple_of(k * step, step), step)
        rows = jnp.concatenate([own_ref[at, :], swapped_ref[at, :]], axis=1)
        logits = lax.dot_general(
            rows, hidden, (((1,), (1,)), ((), ())), preferred_element_type=jnp.float32
        )
        out_ref[at, :] = encode(logits * scale)
        return carry

    lax.fori_loop(0, half // step, add_rows, 0, unroll=True)


def local_call(kernel, name, out, *operands, place=pltpu.VMEM, **more):
    results = [place(shape, dtype) for shape, dtype in out]
    specs = [pl.BlockSpec(memory_space=pltpu.VMEM)] * len(operands)
    operands = [pltpu.with_memory_space_constraint(x, pltpu.VMEM) for x in operands]
    params = pltpu.CompilerParams(vmem_limit_bytes=16 * 2**20)
    return pl.pallas_call(
        kernel, in_specs=specs, out_shape=results, name=name, compiler_params=params, **more
    )(*operands)


def put_stats(out_ref, peak, expsum, target):
    zeros = jnp.zeros((2, LANES), jnp.float32)
    packed = jnp.concatenate([peak, expsum, target, zeros], axis=0)
    for k in range(out_ref.shape[0]):
        out_ref[k] = packed


def two_rows(row):
    return jnp.concatenate([row[:, :LANES], row[:, LANES:]], axis=0)


def sum_kernel(scale, codes_ref, out_ref):
    step = 32

    def add_rows(k, carry):
        at = pl.ds(pl.multiple_of(k * step, step), step)
        out_ref[at, :] = encode(decoded_sum(codes_ref, at) * scale)
        return carry

    lax.fori_loop(0, out_ref.shape[0] // step, add_rows, 0, unroll=4)


def stats_kernel(scale, codes_ref, target_row_ref, out_ref, logits_ref):
    rows, tokens = logits_ref.shape
    step = 32

    def add_rows(k, state):
        peak, target = state
        at = pl.ds(pl.multiple_of(k * step, step), step)
        total = decoded_sum(codes_ref, at) * scale
        logits_ref[at, :] = total
        peak = jnp.maximum(peak, jnp.max(total, axis=0, keepdims=True))
        row = lax.broadcasted_iota(jnp.int32, total.shape, 0) + k * step
        matched = jnp.where(row == target_row_ref[...], total, 0.0)
        return peak, target + jnp.sum(matched, axis=0, keepdims=True)

    start = jnp.full((1, tokens), -jnp.inf, jnp.float32), jnp.zeros((1, tokens), jnp.float32)
    peak, target = lax.fori_loop(0, rows // step, add_rows, start, unroll=True)
    expsum = jnp.sum(jnp.exp(logits_ref[...] - peak), axis=0, keepdims=True)
    put_stats(out_ref, two_rows(peak), two_rows(expsum), two_rows(target))


def combine(parts):
    peaks, expsums, targets = parts[:, 0:2], parts[:, 2:4], parts[:, 4:6]
    peak = jnp.max(peaks, axis=0)
    expsum = jnp.sum(expsums * jnp.exp(peaks - peak), axis=0)
    return peak, expsum, jnp.sum(targets, axis=0)


def combine_kernel(parts_ref, out_ref):
    put_stats(out_ref, *combine(parts_ref[...]))


def finish_kernel(parts_ref, logprob_ref, gap_ref):
    peak, expsum, target = combine(parts_ref[...])
    logprob_ref[...] = target - peak - jnp.log(expsum)
    gap_ref[...] = target - peak


def round_groups(deep, high, tensor):
    def at(z, y, core, rest):
        return ((z * high + y) * 2 + core) * tensor + rest

    one, two = [], []
    for rest in range(tensor):
        for parity in range(2):
            for y in range(high):
                one.append([at(z, y, 0, rest) for z in range(parity, deep, 2)])
        for z in range(deep):
            one.append([at(z, y, 1, rest) for y in range(high)])
        for pair in range(0, deep, 2):
            two.append([at(z, y, 0, rest) for z in (pair, pair + 1) for y in range(high)])
        for y in range(high):
            two.append([at(z, y, 1, rest) for z in range(deep)])
    return one, two


def per_device(hidden, head_weight, targets):
    held = head_weight.shape[0]
    tokens = hidden.shape[0]
    half = held // 2
    deep, high = lax.axis_size(Z), lax.axis_size(Y)
    one, two = round_groups(deep, high, lax.axis_size(TENSOR))
    core = lax.axis_index(CORE)
    own = lax.dynamic_slice_in_dim(head_weight, core * half, half, axis=0)
    swapped = lax.ppermute(pick(head_weight, hidden), CORE, [(0, 1), (1, 0)])
    (codes,) = local_call(
        functools.partial(partial_kernel, 2.0 ** (REACH - 15)),
        "partial",
        [((half, tokens), jnp.bfloat16)],
        own,
        swapped,
        hidden,
    )
    rows = half // high
    z, y = lax.axis_index(Z), lax.axis_index(Y)
    chunk = jnp.where(core == 0, z // 2, y)
    piece = jnp.where(core == 0, z % 2 * high + y, z)
    first_row = lax.axis_index(TENSOR) * held + core * half + chunk * rows + piece * (rows // deep)
    target_row = (targets - first_row).reshape(1, tokens)
    codes, target_row = lax.optimization_barrier((codes, target_row))
    codes = codes.reshape(high, rows, tokens)
    codes = lax.all_to_all(codes, ALL, 0, 0, axis_index_groups=one)
    (codes,) = local_call(
        functools.partial(sum_kernel, 2.0**-2), "sum", [((rows, tokens), jnp.bfloat16)], codes
    )
    codes = codes.reshape(deep, rows // deep, tokens)
    codes = lax.all_to_all(codes, ALL, 0, 0, axis_index_groups=two)
    (stats,) = local_call(
        functools.partial(stats_kernel, 2.0 ** (17 - REACH)),
        "stats",
        [((lax.axis_size(FIRST), 8, LANES), jnp.float32)],
        codes,
        target_row,
        scratch_shapes=[pltpu.VMEM((rows // deep, tokens), jnp.float32)],
    )
    stats = lax.all_to_all(stats, FIRST, 0, 0)
    (stats,) = local_call(
        combine_kernel, "combine", [((lax.axis_size(SECOND), 8, LANES), jnp.float32)], stats
    )
    stats = lax.all_to_all(stats, SECOND, 0, 0)
    logprob, gap = local_call(
        finish_kernel,
        "finish",
        [((2, LANES), jnp.float32)] * 2,
        stats,
        place=jax.ShapeDtypeStruct,
    )
    return logprob.reshape(tokens), gap.reshape(tokens)


def solution(mesh):
    torus = Mesh(mesh.devices.reshape(8, 4, 2, 2, 4), FSDP + TENSOR)
    placed = (P(None, FSDP), P(TENSOR, FSDP), P())
    return jax.shard_map(
        per_device, mesh=torus, in_specs=placed, out_specs=(P(), P()), check_vma=False
    )
```

```python
import functools

import jax
import jax.numpy as jnp
from jax import lax
from jax.experimental import pallas as pl
from jax.experimental.pallas import tpu as pltpu
from jax.sharding import Mesh
from jax.sharding import PartitionSpec as P

Z, Y, CORE, YL, X = "fsdp_0", "fsdp_1", "fsdp_2", "tensor_0", "tensor_1"
FSDP = (Z, Y, CORE)
TENSOR = (YL, X)
ALL = FSDP + TENSOR
FIRST = (CORE, X, YL)
SECOND = (Z, Y)
LANES = 128


REACH = 20


def encode(value):
    cube = value * value * value
    return (cube * jnp.abs(cube)).astype(jnp.bfloat16)


def decode(code):
    code = code.astype(jnp.float32)
    size = jnp.maximum(jnp.abs(code), 2.0**-126)
    return code * jnp.exp2(jnp.log2(size) * (-5 / 6))


def decoded_sum(codes_ref, at):
    total = decode(codes_ref[0, at, :])
    for peer in range(1, codes_ref.shape[0]):
        total = total + decode(codes_ref[peer, at, :])
    return total


def pick_kernel(weight_ref, hidden_ref, out_ref, sems):
    half = weight_ref.shape[0] // 2
    start = (1 - lax.axis_index(CORE)) * half
    rows = pltpu.make_async_copy(
        weight_ref.at[pl.ds(pl.multiple_of(start, half), half)], out_ref.at[:half], sems.at[0]
    )
    features = pltpu.make_async_copy(hidden_ref, out_ref.at[half:], sems.at[1])
    rows.start()
    features.start()
    rows.wait()
    features.wait()


def pick(head_weight, hidden):
    rows = head_weight.shape[0] // 2 + hidden.shape[0]
    return pl.pallas_call(
        pick_kernel,
        in_specs=[pl.BlockSpec(memory_space=pl.ANY)] * 2,
        out_shape=pltpu.VMEM((rows, hidden.shape[1]), hidden.dtype),
        scratch_shapes=[pltpu.SemaphoreType.DMA((2,))],
        name="pick",
    )(head_weight, hidden)


def partial_kernel(scale, own_ref, swapped_ref, hidden_ref, out_ref):
    half, depth = own_ref.shape
    tokens = hidden_ref.shape[0]
    hidden = jnp.concatenate([hidden_ref[...], swapped_ref[half : half + tokens, :]], axis=1)
    step = min(512, half)

    def add_rows(k, carry):
        at = pl.ds(pl.multiple_of(k * step, step), step)
        rows = jnp.concatenate([own_ref[at, :], swapped_ref[at, :]], axis=1)
        logits = lax.dot_general(
            rows, hidden, (((1,), (1,)), ((), ())), preferred_element_type=jnp.float32
        )
        out_ref[at, :] = encode(logits * scale)
        return carry

    lax.fori_loop(0, half // step, add_rows, 0, unroll=True)


def local_call(kernel, name, out, *operands, place=pltpu.VMEM, **more):
    results = [place(shape, dtype) for shape, dtype in out]
    specs = [pl.BlockSpec(memory_space=pltpu.VMEM)] * len(operands)
    operands = [pltpu.with_memory_space_constraint(x, pltpu.VMEM) for x in operands]
    params = pltpu.CompilerParams(vmem_limit_bytes=16 * 2**20)
    return pl.pallas_call(
        kernel, in_specs=specs, out_shape=results, name=name, compiler_params=params, **more
    )(*operands)


def put_stats(out_ref, peak, expsum, target):
    zeros = jnp.zeros((2, LANES), jnp.float32)
    packed = jnp.concatenate([peak, expsum, target, zeros], axis=0)
    for k in range(out_ref.shape[0]):
        out_ref[k] = packed


def two_rows(row):
    return jnp.concatenate([row[:, :LANES], row[:, LANES:]], axis=0)


def sum_kernel(scale, codes_ref, out_ref):
    step = 32

    def add_rows(k, carry):
        at = pl.ds(pl.multiple_of(k * step, step), step)
        out_ref[at, :] = encode(decoded_sum(codes_ref, at) * scale)
        return carry

    lax.fori_loop(0, out_ref.shape[0] // step, add_rows, 0, unroll=4)


def stats_kernel(scale, codes_ref, target_row_ref, out_ref, logits_ref):
    rows, tokens = logits_ref.shape
    step = 32

    def add_rows(k, state):
        peak, target = state
        at = pl.ds(pl.multiple_of(k * step, step), step)
        total = decoded_sum(codes_ref, at) * scale
        logits_ref[at, :] = total
        peak = jnp.maximum(peak, jnp.max(total, axis=0, keepdims=True))
        row = lax.broadcasted_iota(jnp.int32, total.shape, 0) + k * step
        matched = jnp.where(row == target_row_ref[...], total, 0.0)
        return peak, target + jnp.sum(matched, axis=0, keepdims=True)

    start = jnp.full((1, tokens), -jnp.inf, jnp.float32), jnp.zeros((1, tokens), jnp.float32)
    peak, target = lax.fori_loop(0, rows // step, add_rows, start, unroll=True)
    expsum = jnp.sum(jnp.exp(logits_ref[...] - peak), axis=0, keepdims=True)
    put_stats(out_ref, two_rows(peak), two_rows(expsum), two_rows(target))


def combine(parts):
    peaks, expsums, targets = parts[:, 0:2], parts[:, 2:4], parts[:, 4:6]
    peak = jnp.max(peaks, axis=0)
    expsum = jnp.sum(expsums * jnp.exp(peaks - peak), axis=0)
    return peak, expsum, jnp.sum(targets, axis=0)


def combine_kernel(parts_ref, out_ref):
    put_stats(out_ref, *combine(parts_ref[...]))


def finish_kernel(parts_ref, logprob_ref, gap_ref):
    peak, expsum, target = combine(parts_ref[...])
    logprob_ref[...] = target - peak - jnp.log(expsum)
    gap_ref[...] = target - peak


def round_groups(deep, high, tensor):
    def at(z, y, core, rest):
        return ((z * high + y) * 2 + core) * tensor + rest

    one, two = [], []
    for rest in range(tensor):
        for parity in range(2):
            for y in range(high):
                one.append([at(z, y, 0, rest) for z in range(parity, deep, 2)])
        for z in range(deep):
            one.append([at(z, y, 1, rest) for y in range(high)])
        for pair in range(0, deep, 2):
            two.append([at(z, y, 0, rest) for z in (pair, pair + 1) for y in range(high)])
        for y in range(high):
            two.append([at(z, y, 1, rest) for z in range(deep)])
    return one, two


def per_device(hidden, head_weight, targets):
    held = head_weight.shape[0]
    tokens = hidden.shape[0]
    half = held // 2
    deep, high = lax.axis_size(Z), lax.axis_size(Y)
    one, two = round_groups(deep, high, lax.axis_size(TENSOR))
    core = lax.axis_index(CORE)
    own = lax.dynamic_slice_in_dim(head_weight, core * half, half, axis=0)
    swapped = lax.ppermute(pick(head_weight, hidden), CORE, [(0, 1), (1, 0)])
    (codes,) = local_call(
        functools.partial(partial_kernel, 2.0 ** (REACH - 15)),
        "partial",
        [((half, tokens), jnp.bfloat16)],
        own,
        swapped,
        hidden,
    )
    rows = half // high
    z, y = lax.axis_index(Z), lax.axis_index(Y)
    chunk = jnp.where(core == 0, z // 2, y)
    piece = jnp.where(core == 0, z % 2 * high + y, z)
    first_row = lax.axis_index(TENSOR) * held + core * half + chunk * rows + piece * (rows // deep)
    target_row = (targets - first_row).reshape(1, tokens)
    codes, target_row = lax.optimization_barrier((codes, target_row))
    codes = codes.reshape(high, rows, tokens)
    codes = lax.all_to_all(codes, ALL, 0, 0, axis_index_groups=one)
    (codes,) = local_call(
        functools.partial(sum_kernel, 2.0**-2), "sum", [((rows, tokens), jnp.bfloat16)], codes
    )
    codes = codes.reshape(deep, rows // deep, tokens)
    codes = lax.all_to_all(codes, ALL, 0, 0, axis_index_groups=two)
    (stats,) = local_call(
        functools.partial(stats_kernel, 2.0 ** (17 - REACH)),
        "stats",
        [((lax.axis_size(FIRST), 8, LANES), jnp.float32)],
        codes,
        target_row,
        scratch_shapes=[pltpu.VMEM((rows // deep, tokens), jnp.float32)],
    )
    stats = lax.all_to_all(stats, FIRST, 0, 0)
    (stats,) = local_call(
        combine_kernel, "combine", [((lax.axis_size(SECOND), 8, LANES), jnp.float32)], stats
    )
    stats = lax.all_to_all(stats, SECOND, 0, 0)
    logprob, gap = local_call(
        finish_kernel,
        "finish",
        [((2, LANES), jnp.float32)] * 2,
        stats,
        place=jax.ShapeDtypeStruct,
    )
    return logprob.reshape(tokens), gap.reshape(tokens)


def solution(mesh):
    torus = Mesh(mesh.devices.reshape(8, 4, 2, 2, 4), FSDP + TENSOR)
    placed = (P(None, FSDP), P(TENSOR, FSDP), P())
    return jax.shard_map(
        per_device, mesh=torus, in_specs=placed, out_specs=(P(), P()), check_vma=False
    )
```
